32 devices in a mesh: groups: 2 (over y), blk: 4 (over z), tok: 4 (over x, core).
Axes of the slice: x: 2, y: 2, z: 4, core: 2. Of those that a mesh axis runs over, the one named last changes fastest.
Arguments:
- tokens: bfloat16 [2048, 3584], P(('groups', 'blk', 'tok')), parts along dimension 0, may hold values from -6 to 6
- expert_ids: int32 [2048, 1], P(('groups', 'blk', 'tok')), parts along dimension 0, may hold values from 0 to 1; in each aligned block of 256 rows (0 to 255, 256 to 511, ...) at most 192 rows name the same one
- gate_values: float32 [2048, 1], P(('groups', 'blk', 'tok')), parts along dimension 0, may hold values from 0.2 to 1
- w_gate: bfloat16 [2, 3584, 1024], P(None, 'blk', 'tok'), may hold values from -0.09375 to 0.09375
- w_up: bfloat16 [2, 3584, 1024], P(None, 'blk', 'tok'), may hold values from -0.09375 to 0.09375
- w_down: bfloat16 [2, 1024, 3584], P(None, 'tok', 'blk'), may hold values from -0.1875 to 0.1875
Outputs:
- mixed: bfloat16 [2048, 3584], P(('groups', 'blk', 'tok')), parts along dimension 0
The draws below stay inside these ranges and needn't reach their ends.
There are 2 independent parts, one for each index of `groups`. The reference program is written for one: setup_inputs(seed, part) draws one part's arguments, and reference() takes and returns one part's arrays. A program takes and returns all parts, laid end to end along the dimension named above; an argument that names none is the same for every part. Nothing has to cross between parts.
Inputs may be any that keep to these rules, and one draw needn't show every extreme that they name: `expert_ids`: in each aligned block of 256 rows (the tokens of one index of blk), no expert is named by more than 192 rows, and in every draw some expert reaches 192 in some block.
All inputs are finite; a program needn't handle non-finite values.
Results may differ from the reference program's by a relative error of at most 0.005.
Values may be sent and summed in bfloat16 or wider, within the bound.
A program may use at most 64 MiB of HBM per device.

```python
import math
import jax
import jax.numpy as jnp
import numpy as np
from jax import lax

D = 3584
FF = 1024
EXPERTS = 2
TOPK = 1
GROUP = 256
CAP = 192
TOKENS = 1024


def steps_of(key, shape, cuts, least, high):
    def one(axis_at, shards_of):
        heights = jax.random.uniform(jax.random.fold_in(jax.random.fold_in(key, 6), axis_at), (shards_of,), jnp.float32, least / len(cuts), high / len(cuts))
        return jnp.repeat(jnp.exp(heights), shape[axis_at] // shards_of).reshape((-1,) + (1,) * (len(shape) - axis_at - 1))

    gain = one(*cuts[0])
    for cut in cuts[1:]:
        gain = gain * one(*cut)
    return gain


def assign_block(stream_key, own, number, rows, amount, top, reach, slope):
    sequence = jax.random.permutation(stream_key, amount)
    crowded, ordinary = shares(amount, rows * top, reach, slope, True), shares(amount, rows * top, reach, slope, False)
    places = jnp.arange(amount)

    def named(tallies, turn):
        used = int((tallies > 0).sum())
        fixed = max(1, used // 4)
        moved = fixed + (places - fixed + turn * (used - fixed)) % max(1, amount - fixed)
        return jnp.zeros((amount,), jnp.int32).at[sequence[jnp.where(places < fixed, places, moved)]].set(jnp.asarray(tallies, jnp.int32))

    tallies = jnp.where(number % 4 == 0, named(crowded, number // 4), named(ordinary, number - number // 4 - 1))
    mixed = jax.random.permutation(jax.random.fold_in(own, 3), amount)
    source_of, taker = mixed[0:amount // 2 * 2:2], mixed[1:amount // 2 * 2:2]
    margin = jnp.minimum(tallies[source_of] - 1, reach - tallies[taker]) // 2
    margin = jnp.where((source_of == sequence[0]) | (taker == sequence[0]) | (tallies[taker] == 0), 0, jnp.maximum(margin, 0))
    moved = jax.random.randint(jax.random.fold_in(own, 4), (amount // 2,), 0, 1 << 20) % (margin + 1)
    tallies = tallies.at[source_of].add(-moved).at[taker].add(moved)
    labels = jnp.searchsorted(jnp.cumsum(tallies), jnp.arange(rows * top), side="right").astype(jnp.int32)
    listing = labels.reshape(top, rows).T
    listing = listing[jax.random.permutation(jax.random.fold_in(own, 1), rows)]
    turn = jax.random.randint(jax.random.fold_in(own, 2), (rows, 1), 0, top)
    return jnp.take_along_axis(listing, (jnp.arange(top)[None, :] + turn) % top, axis=1)


def shares(amount, total, most, lean, full):
    portions = [(1 << 20) // math.isqrt(rank ** lean) + 1 for rank in range(1, amount + 1)]
    largest = most if full else min(most, max(-(-total // amount), total * portions[0] // sum(portions)))
    least = 1 if total - largest >= amount - 1 else 0
    given, spare = [largest] + [least] * (amount - 1), total - largest - least * (amount - 1)
    while spare > 0:
        candidates = [i for i in range(1, amount) if given[i] < largest] or [i for i in range(1, amount) if given[i] < most]
        whole, budget = sum([portions[i] for i in candidates]), spare
        for i in candidates:
            extra = min(most - given[i], max(1, budget * portions[i] // whole), spare)
            given[i] = given[i] + extra
            spare = spare - extra
    return np.array(given)


def gaussian(stream_key, dims, width, limit, cuts=(), kind=jnp.bfloat16):
    drawn = jax.random.normal(stream_key, dims, jnp.float32) * width
    if len(cuts) > 0:
        drawn = steps_of(stream_key, dims, cuts, -0.22, 0.18) * drawn
    return jnp.clip(drawn, min=-limit, max=limit).astype(kind)


def setup_inputs(seed: int = 0, part: int = 0) -> dict:
    streams_of = jax.random.split(jax.random.key(seed), 7)
    own_keys = jax.random.split(jax.random.fold_in(streams_of[6], part), 7)
    tokens = gaussian(own_keys[0], (TOKENS, D), 1.0, 6.0, ((0, 16),))
    expert_ids_keys = jax.random.split(jax.random.fold_in(own_keys[1], 1), TOKENS // GROUP)
    expert_ids_turns = jax.random.permutation(jax.random.fold_in(own_keys[1], 3), TOKENS // GROUP)
    expert_ids = jax.vmap(lambda own, number: assign_block(jax.random.fold_in(own_keys[1], 2), own, number, GROUP, EXPERTS, TOPK, CAP, 2))(expert_ids_keys, expert_ids_turns).reshape((TOKENS, TOPK))
    gate_values = jnp.clip(0.2 + 0.8 * jax.random.uniform(own_keys[2], (TOKENS, TOPK), jnp.float32) ** steps_of(own_keys[2], (TOKENS, TOPK), ((0, 16),), -0.2, 0.2), 0.2, 1.0)
    w_gate = gaussian(streams_of[3], (EXPERTS, D, FF), D ** -0.5, 0.09375, ((1, 4), (2, 4)))
    w_up = gaussian(streams_of[4], (EXPERTS, D, FF), D ** -0.5, 0.09375, ((1, 4), (2, 4)))
    w_down = gaussian(streams_of[5], (EXPERTS, FF, D), FF ** -0.5, 0.1875, ((1, 4), (2, 4)))
    return {"tokens": tokens, "expert_ids": expert_ids, "gate_values": gate_values, "w_gate": w_gate, "w_up": w_up, "w_down": w_down}


block_rows = 512


def expert_block(token_block, gate_weight, up_weight, down_weight):
    gate = jnp.dot(token_block, gate_weight, preferred_element_type=jnp.float32)
    up = jnp.dot(token_block, up_weight, preferred_element_type=jnp.float32)
    hidden = (jax.nn.silu(gate) * up).astype(jnp.bfloat16)
    return jnp.dot(hidden, down_weight, preferred_element_type=jnp.float32)


def reference(tokens, expert_ids, gate_values, w_gate, w_up, w_down):
    count_tokens = tokens.shape[0]
    routes = expert_ids[:, 0].astype(jnp.int32)
    onehot = (routes[:, None] == jnp.arange(EXPERTS, dtype=jnp.int32)[None, :]).astype(jnp.int32)
    slot_rank = jnp.sum((jnp.cumsum(onehot, axis=0) - onehot) * onehot, axis=1).astype(jnp.int32)
    counts = jnp.sum(onehot, axis=0).astype(jnp.int32)
    padded = ((counts + block_rows - 1) // block_rows) * block_rows
    starts = (jnp.cumsum(padded) - padded).astype(jnp.int32)
    destination = (jnp.take(starts, routes) + slot_rank).astype(jnp.int32)
    num_blocks = (count_tokens + block_rows - 1) // block_rows + EXPERTS
    total_slots = num_blocks * block_rows
    slot_token = jnp.zeros((total_slots,), jnp.int32).at[destination].set(jnp.arange(count_tokens, dtype=jnp.int32))
    block_start = jnp.arange(num_blocks, dtype=jnp.int32) * block_rows
    block_expert = jnp.sum((starts[None, :] <= block_start[:, None]).astype(jnp.int32), axis=1) - 1
    block_expert = jnp.clip(block_expert, 0, EXPERTS - 1).astype(jnp.int32)

    def run_block(args):
        indices, expert = args
        token_block = jnp.take(tokens, indices, axis=0)
        return expert_block(token_block, w_gate[expert], w_up[expert], w_down[expert])

    outputs = lax.map(run_block, (slot_token.reshape(num_blocks, block_rows), block_expert))
    flat_rows = outputs.reshape(total_slots, tokens.shape[1])
    expert_out = jnp.take(flat_rows, destination, axis=0)
    return (gate_values[:, 0:1] * expert_out).astype(jnp.bfloat16)
```

```python
import functools

import jax
import jax.numpy as jnp
from jax import lax
from jax.experimental import pallas as pl
from jax.experimental.pallas import tpu as pltpu
from jax.sharding import PartitionSpec as P

LANES = 128
SUBLANES = 8


def gathered_body(tokens, expert_ids, gate_values, w_gate, w_up, w_down):
    group_rows = lax.all_gather(tokens, "tok", axis=0, tiled=True)
    group_routes = lax.all_gather(expert_ids, "tok", axis=0, tiled=True)[:, 0]
    experts = w_gate.shape[0]
    count_rows = group_rows.shape[0]
    capacity = 3 * count_rows // 4
    expert_range = jnp.arange(experts, dtype=jnp.int32)
    onehot = (group_routes[:, None] == expert_range[None, :]).astype(jnp.int32)
    slot_rank = jnp.sum((jnp.cumsum(onehot, axis=0) - onehot) * onehot, axis=1)
    expert_match = group_routes[None, None, :] == expert_range[:, None, None]
    slot_match = slot_rank[None, None, :] == jnp.arange(capacity, dtype=jnp.int32)[None, :, None]
    dispatch = (expert_match & slot_match).astype(jnp.bfloat16)
    slots = jnp.einsum(
        "esg,gd->esd", dispatch, group_rows, preferred_element_type=jnp.float32
    ).astype(jnp.bfloat16)

    def add_part(weights):
        return jnp.einsum("esd,edf->esf", slots, weights, preferred_element_type=jnp.float32)

    gate_sum = add_part(lax.all_gather(w_gate, "blk", axis=1, tiled=True))
    up_sum = add_part(lax.all_gather(w_up, "blk", axis=1, tiled=True))
    hidden = (jax.nn.silu(gate_sum) * up_sum).astype(jnp.bfloat16)
    slot_out = jnp.einsum(
        "esf,efd->esd",
        hidden,
        lax.all_gather(w_down, "blk", axis=2, tiled=True),
        preferred_element_type=jnp.float32,
    )
    flat_rows = slot_out.reshape(experts * capacity, slot_out.shape[2])
    position = group_routes * capacity + slot_rank
    partial_value = jnp.take(flat_rows, position, axis=0)
    summed = lax.psum_scatter(partial_value, "tok", scatter_dimension=0, tiled=True)
    return (gate_values * summed).astype(jnp.bfloat16)


def kernel(
    nb, nt, tok_hbm, meta_hbm, wg_hbm, wu_hbm, wd_hbm, out_ref,
    tok, meta, wg, wu, wd, xs, part_own, part_send, part_recv, hid, ys, ycore, yx_send, yx_recv, fin_send,
    local_sem, z_send, z_recv, x_send, x_recv, c_send, c_recv, f_send, f_recv, m_send, m_recv,
    p_send, p_recv, h_send, h_recv, yc_send_sem, yc_recv_sem, yx_send_sem, yx_recv_sem, o_send, o_recv,
):
    g, b, t = lax.axis_index("groups"), lax.axis_index("blk"), lax.axis_index("tok")
    rows, width = tok.shape[0], xs.shape[3]
    experts, ff = wg.shape[0], wg.shape[2]
    half = nt // 2
    f32, bf16 = jnp.float32, jnp.bfloat16
    pair = t + 1 - 2 * lax.rem(t, 2)

    def blk(k):
        return lax.rem(b + k + nb, nb)

    def tk(base, j):
        return lax.rem(base + j + nt, nt)

    def cols(block):
        return pl.ds(pl.multiple_of(block * width, LANES), width)

    def remote(src, dst, send, recv, to_b, to_t):
        copy = pltpu.make_async_remote_copy(
            src_ref=src, dst_ref=dst, send_sem=send, recv_sem=recv,
            device_id=(g, to_b, to_t), device_id_type=pl.DeviceIdType.MESH,
        )
        copy.start()
        sends.append(copy)

    def arrived(dst, recv):
        pltpu.make_async_copy(dst, dst, recv).wait()

    sends = []
    local = [
        pltpu.make_async_copy(tok_hbm, tok, local_sem.at[0]),
        pltpu.make_async_copy(meta_hbm, meta.at[b, t], local_sem.at[1]),
        pltpu.make_async_copy(tok_hbm.at[:, cols(b)], xs.at[b, t], local_sem.at[2]),
        pltpu.make_async_copy(wg_hbm, wg, local_sem.at[3]),
        pltpu.make_async_copy(wu_hbm, wu, local_sem.at[4]),
        pltpu.make_async_copy(wd_hbm, wd, local_sem.at[5]),
    ]
    for copy in local:
        copy.start()

    barrier = pltpu.get_barrier_semaphore()
    for k in range(nb):
        for j in range(nt):
            if k or j:
                pl.semaphore_signal(
                    barrier, inc=1, device_id=(g, blk(k), tk(t, j)),
                    device_id_type=pl.DeviceIdType.MESH,
                )
    pl.semaphore_wait(barrier, nb * nt - 1)

    order = [0]
    for k in range(1, nb // 2 + 1):
        order += [k] if 2 * k == nb else [k, nb - k]
    others = order[1:]

    local[0].wait()
    for k in others:
        remote(tok.at[:, cols(blk(k))], xs.at[b, t], z_send.at[k], z_recv.at[k], blk(k), t)
    local[1].wait()
    for k in order:
        for j in range(nt):
            if k or j:
                remote(meta.at[b, t], meta.at[b, t], m_send.at[k, j], m_recv.at[k, j], blk(k), tk(t, j))
    local[2].wait()

    def spread(k):
        source = blk(-k)
        if k:
            arrived(xs.at[source, t], z_recv.at[k])
        mine = xs.at[source, t]
        for j in range(1, half):
            remote(mine, mine, x_send.at[k, j], x_recv.at[k, j], b, tk(t, 2 * j))
        remote(mine, mine, c_send.at[k], c_recv.at[k], b, pair)

    def pass_on(k):
        source = blk(-k)
        for j in range(1, half):
            theirs = xs.at[source, tk(t, -2 * j)]
            arrived(theirs, x_recv.at[k, j])
            remote(theirs, theirs, f_send.at[k, j], f_recv.at[k, j], b, pair)

    def column(k, row):
        flat = meta[blk(-k)].reshape(nt * SUBLANES, LANES)
        turned = jnp.transpose(flat)
        return jnp.concatenate(
            [turned[:rows, SUBLANES * i + row:SUBLANES * i + row + 1] for i in range(nt)], axis=0
        )

    def contract(k):
        source = blk(-k)
        arrived(xs.at[source, pair], c_recv.at[k])
        for j in range(1, half):
            arrived(xs.at[source, tk(pair, -2 * j)], f_recv.at[k, j])
        for j in range(nt):
            if k or j:
                arrived(meta.at[source, tk(t, -j)], m_recv.at[k, j])
        if k == 0:
            local[3].wait()
            local[4].wait()
        routes = column(k, 0)
        x = xs[source].reshape(nt * rows, width)
        for at, weights in ((0, wg), (ff, wu)):
            total = None
            for e in range(experts):
                value = jnp.dot(x, weights[e], preferred_element_type=f32)
                total = value if e == 0 else jnp.where(routes == e, value, total)
            if k == 0:
                part_own[:, at:at + ff] = total
            else:
                part_send[k, :, at:at + ff] = total.astype(bf16)
        if k:
            remote(part_send.at[k], part_recv.at[k], p_send.at[k], p_recv.at[k], source, t)

    stage = [(spread, 0), (pass_on, 1), (contract, 2)]
    for step in range(nb + 2):
        for run, lag in stage:
            at = step - lag
            if 0 <= at < nb:
                run(order[at])

    for k in others:
        arrived(part_recv.at[k], p_recv.at[k])
    gate = part_own[:, :ff]
    up = part_own[:, ff:]
    for k in others:
        gate = gate + part_recv[k, :, :ff].astype(f32)
        up = up + part_recv[k, :, ff:].astype(f32)
    hid[b] = (gate / (1.0 + jnp.exp(-gate)) * up * column(0, 1)).astype(bf16)
    for k in others:
        remote(hid.at[b], hid.at[b], h_send.at[k], h_recv.at[k], blk(k), t)

    def expand(k):
        source = blk(-k)
        if k:
            arrived(hid.at[source], h_recv.at[k])
        else:
            local[5].wait()
        routes = column(k, 0)
        h = hid[source].astype(f32)
        routed = jnp.concatenate(
            [jnp.where(routes == e, h, 0.0).astype(bf16) for e in range(experts)], axis=1
        )
        ys[k] = jnp.dot(routed, wd[...].reshape(experts * ff, width), preferred_element_type=f32)
        for j in reversed(range(half)):
            remote(
                ys.at[k, rows_of(tk(pair, 2 * j))], ycore.at[k, j],
                yc_send_sem.at[k, j], yc_recv_sem.at[k, j], b, pair,
            )

    def rows_of(index):
        return pl.ds(pl.multiple_of(index * rows, SUBLANES), rows)

    def exchange(k):
        for j in range(1, half):
            arrived(ycore.at[k, j], yc_recv_sem.at[k, j])
            total = ys[k, rows_of(tk(t, 2 * j)), :] + ycore[k, j]
            yx_send[k, j] = total.astype(bf16)
            remote(
                yx_send.at[k, j], yx_recv.at[k, j],
                yx_send_sem.at[k, j], yx_recv_sem.at[k, j], b, tk(t, 2 * j),
            )

    def finish(k):
        arrived(ycore.at[k, 0], yc_recv_sem.at[k, 0])
        total = ys[k, rows_of(t), :] + ycore[k, 0]
        for j in range(1, half):
            arrived(yx_recv.at[k, j], yx_recv_sem.at[k, j])
            total = total + yx_recv[k, j].astype(f32)
        if k:
            fin_send[k] = total.astype(bf16)
            remote(fin_send.at[k], out_ref.at[:, cols(b)], o_send.at[k], o_recv.at[k], blk(-k), t)
        else:
            out_ref[:, cols(b)] = total.astype(bf16)

    stage = [(expand, 0), (exchange, 1), (finish, 2)]
    for step in range(nb + 2):
        for run, lag in stage:
            at = step - lag
            if 0 <= at < nb:
                run(order[at])

    for k in others:
        arrived(out_ref.at[:, cols(blk(k))], o_recv.at[k])
    for copy in sends:
        copy.wait_send()


def stationary_body(nb, nt, tokens, expert_ids, gate_values, w_gate, w_up, w_down):
    rows, features = tokens.shape
    experts, width, ff = w_gate.shape
    f32, bf16 = jnp.float32, jnp.bfloat16
    lines = jnp.stack([expert_ids[:, 0].astype(f32), gate_values[:, 0]])
    meta = jnp.pad(lines, ((0, SUBLANES - 2), (0, LANES - rows)))
    block, half = nt * rows, nt // 2
    dma = pltpu.SemaphoreType.DMA
    anywhere = pl.BlockSpec(memory_space=pl.ANY)
    return pl.pallas_call(
        functools.partial(kernel, nb, nt),
        out_shape=jax.ShapeDtypeStruct((rows, features), bf16),
        in_specs=[anywhere] * 5,
        out_specs=pl.BlockSpec(memory_space=pltpu.VMEM),
        scratch_shapes=[
            pltpu.VMEM((rows, features), bf16),
            pltpu.VMEM((nb, nt, SUBLANES, LANES), f32),
            pltpu.VMEM(w_gate.shape, bf16),
            pltpu.VMEM(w_up.shape, bf16),
            pltpu.VMEM(w_down.shape, bf16),
            pltpu.VMEM((nb, nt, rows, width), bf16),
            pltpu.VMEM((block, 2 * ff), f32),
            pltpu.VMEM((nb, block, 2 * ff), bf16),
            pltpu.VMEM((nb, block, 2 * ff), bf16),
            pltpu.VMEM((nb, block, ff), bf16),
            pltpu.VMEM((nb, block, width), f32),
            pltpu.VMEM((nb, half, rows, width), f32),
            pltpu.VMEM((nb, half, rows, width), bf16),
            pltpu.VMEM((nb, half, rows, width), bf16),
            pltpu.VMEM((nb, rows, width), bf16),
            dma((6,)),
            dma((nb,)), dma((nb,)),
            dma((nb, half)), dma((nb, half)),
            dma((nb,)), dma((nb,)),
            dma((nb, half)), dma((nb, half)),
            dma((nb, nt)), dma((nb, nt)),
            dma((nb,)), dma((nb,)),
            dma((nb,)), dma((nb,)),
            dma((nb, half)), dma((nb, half)),
            dma((nb, half)), dma((nb, half)),
            dma((nb,)), dma((nb,)),
        ],
        compiler_params=pltpu.CompilerParams(collective_id=0, has_side_effects=True),
    )(tokens, meta, w_gate, w_up, w_down)


def solution(mesh):
    nb, nt = mesh.shape["blk"], mesh.shape["tok"]

    def body(tokens, expert_ids, gate_values, w_gate, w_up, w_down):
        rows = tokens.shape[0]
        width, ff = w_gate.shape[1], w_gate.shape[2]
        fits = width % LANES == 0 and ff % LANES == 0 and rows % 16 == 0 and rows <= LANES
        if fits and nt % 2 == 0 and nb <= 8:
            return stationary_body(nb, nt, tokens, expert_ids, gate_values, w_gate, w_up, w_down)
        return gathered_body(tokens, expert_ids, gate_values, w_gate, w_up, w_down)

    return jax.shard_map(
        body,
        mesh=mesh,
        in_specs=(
            P(("groups", "blk", "tok"), None),
            P(("groups", "blk", "tok"), None),
            P(("groups", "blk", "tok"), None),
            P(None, "blk", "tok"),
            P(None, "blk", "tok"),
            P(None, "tok", "blk"),
        ),
        out_specs=P(("groups", "blk", "tok"), None),
        check_vma=False,
    )
```

```python
import functools

import jax
import jax.numpy as jnp
from jax import lax
from jax.experimental import pallas as pl
from jax.experimental.pallas import tpu as pltpu
from jax.sharding import PartitionSpec as P

LANES = 128
SUBLANES = 8
CHUNKS = 2


def gathered_body(tokens, expert_ids, gate_values, w_gate, w_up, w_down):
    group_rows = lax.all_gather(tokens, "tok", axis=0, tiled=True)
    group_routes = lax.all_gather(expert_ids, "tok", axis=0, tiled=True)[:, 0]
    experts = w_gate.shape[0]
    count_rows = group_rows.shape[0]
    capacity = 3 * count_rows // 4
    expert_range = jnp.arange(experts, dtype=jnp.int32)
    onehot = (group_routes[:, None] == expert_range[None, :]).astype(jnp.int32)
    slot_rank = jnp.sum((jnp.cumsum(onehot, axis=0) - onehot) * onehot, axis=1)
    expert_match = group_routes[None, None, :] == expert_range[:, None, None]
    slot_match = slot_rank[None, None, :] == jnp.arange(capacity, dtype=jnp.int32)[None, :, None]
    dispatch = (expert_match & slot_match).astype(jnp.bfloat16)
    slots = jnp.einsum(
        "esg,gd->esd", dispatch, group_rows, preferred_element_type=jnp.float32
    ).astype(jnp.bfloat16)

    def add_part(weights):
        return jnp.einsum("esd,edf->esf", slots, weights, preferred_element_type=jnp.float32)

    gate_sum = add_part(lax.all_gather(w_gate, "blk", axis=1, tiled=True))
    up_sum = add_part(lax.all_gather(w_up, "blk", axis=1, tiled=True))
    hidden = (jax.nn.silu(gate_sum) * up_sum).astype(jnp.bfloat16)
    slot_out = jnp.einsum(
        "esf,efd->esd",
        hidden,
        lax.all_gather(w_down, "blk", axis=2, tiled=True),
        preferred_element_type=jnp.float32,
    )
    flat_rows = slot_out.reshape(experts * capacity, slot_out.shape[2])
    position = group_routes * capacity + slot_rank
    partial_value = jnp.take(flat_rows, position, axis=0)
    summed = lax.psum_scatter(partial_value, "tok", scatter_dimension=0, tiled=True)
    return (gate_values * summed).astype(jnp.bfloat16)


def kernel(
    nb, nt, tok_hbm, ids_ref, values_ref, wg_hbm, wu_hbm, wd_hbm, out_ref,
    tok, meta, wg, wu, wd, xs, part, part_send, part_recv, hid, ys, ycore, yx_send, yx_recv, fin_send,
    local_sem, z_send, z_recv, x_send, x_recv, c_send, c_recv, f_send, f_recv, m_send, m_recv,
    p_send, p_recv, h_send, h_recv, yc_send_sem, yc_recv_sem, yx_send_sem, yx_recv_sem, o_send, o_recv,
):
    g, b, t = lax.axis_index("groups"), lax.axis_index("blk"), lax.axis_index("tok")
    rows, width = tok.shape[0], xs.shape[3]
    experts, ff = wg.shape[0], wg.shape[2]
    half = nt // 2
    f32, bf16 = jnp.float32, jnp.bfloat16
    pair = t + 1 - 2 * lax.rem(t, 2)

    outer = lax.rem((b + 1) // 2 + 1, 2)
    piece = nt * rows // CHUNKS

    def blk(k):
        low, high = lax.rem(b, 2), b // 2
        low = 1 - low if k % 2 else low
        high = 1 - high if k // 2 else high
        return 2 * high + low

    def chunk(c):
        return pl.ds(c * piece, piece)

    def tk(base, j):
        return lax.rem(base + j + nt, nt)

    def cols(block):
        return pl.ds(pl.multiple_of(block * width, LANES), width)

    def remote(src, dst, send, recv, to_b, to_t):
        copy = pltpu.make_async_remote_copy(
            src_ref=src, dst_ref=dst, send_sem=send, recv_sem=recv,
            device_id=(g, to_b, to_t), device_id_type=pl.DeviceIdType.MESH,
        )
        copy.start()
        sends.append(copy)

    def arrived(dst, recv):
        pltpu.make_async_copy(dst, dst, recv).wait()

    sends = []
    local = [
        pltpu.make_async_copy(tok_hbm, tok, local_sem.at[0]),
        pltpu.make_async_copy(tok_hbm.at[:, cols(b)], xs.at[b, t], local_sem.at[1]),
        pltpu.make_async_copy(wd_hbm, wd, local_sem.at[2]),
        pltpu.make_async_copy(wg_hbm, wg, local_sem.at[3]),
        pltpu.make_async_copy(wu_hbm, wu, local_sem.at[4]),
    ]
    for copy in local:
        copy.start()

    meta[b, t] = jnp.zeros((SUBLANES, LANES), f32)
    meta[b, t, 0:1, :rows] = ids_ref[...].astype(f32)
    meta[b, t, 1:2, :rows] = values_ref[...]

    barrier = pltpu.get_barrier_semaphore()
    for k in range(nb):
        for j in range(nt):
            if k or j:
                pl.semaphore_signal(
                    barrier, inc=1, device_id=(g, blk(k), tk(t, j)),
                    device_id_type=pl.DeviceIdType.MESH,
                )
    pl.semaphore_wait(barrier, nb * nt - 1)

    order = list(range(nb))
    others = order[1:]

    local[0].wait()
    for k in others:
        remote(tok.at[:, cols(blk(k))], xs.at[b, t], z_send.at[k], z_recv.at[k], blk(k), t)
    for k in order:
        for j in range(nt):
            if k or j:
                remote(meta.at[b, t], meta.at[b, t], m_send.at[k, j], m_recv.at[k, j], blk(k), tk(t, j))
    local[1].wait()

    def spread(k):
        source = blk(k)
        if k:
            arrived(xs.at[source, t], z_recv.at[k])
        mine = xs.at[source, t]
        for j in range(1, half):
            remote(mine, mine, x_send.at[k, j], x_recv.at[k, j], b, tk(t, 2 * j))
        remote(mine, mine, c_send.at[k], c_recv.at[k], b, pair)

    def pass_on(k):
        source = blk(k)
        for j in range(1, half):
            theirs = xs.at[source, tk(t, -2 * j)]
            arrived(theirs, x_recv.at[k, j])
            remote(theirs, theirs, f_send.at[k, j], f_recv.at[k, j], b, pair)

    def column(k, row):
        flat = meta[blk(k)].reshape(nt * SUBLANES, LANES)
        turned = jnp.transpose(flat)
        return jnp.concatenate(
            [turned[:rows, SUBLANES * i + row:SUBLANES * i + row + 1] for i in range(nt)], axis=0
        )

    def contract(k):
        source = blk(k)
        arrived(xs.at[source, pair], c_recv.at[k])
        for j in range(1, half):
            arrived(xs.at[source, tk(pair, -2 * j)], f_recv.at[k, j])
        for j in range(nt):
            if k or j:
                arrived(meta.at[source, tk(t, -j)], m_recv.at[k, j])
        if k == 0:
            local[3].wait()
            local[4].wait()
        routes = column(k, 0)
        x = xs[source].reshape(nt * rows, width)
        for at, weights in ((0, wg), (ff, wu)):
            total = None
            for e in range(experts):
                value = jnp.dot(x, weights[e], preferred_element_type=f32)
                total = value if e == 0 else jnp.where(routes == e, value, total)
            part[k, :, at:at + ff] = total
        if k == 1:
            part_send[k] = part[k].astype(bf16)
            for c in range(CHUNKS):
                send_part(k, c).start()
        elif k:
            @pl.when(outer == 1)
            def _():
                part_send[k] = part[k].astype(bf16)
                for c in range(CHUNKS):
                    send_part(k, c).start()

    def send_part(k, c):
        slot = 0 if k == 1 else outer * (5 - k) + 1 - outer
        target = blk(1) if k == 1 else outer * blk(1) + (1 - outer) * blk(k)
        return pltpu.make_async_remote_copy(
            src_ref=part_send.at[k, chunk(c)], dst_ref=part_recv.at[slot, chunk(c)],
            send_sem=p_send.at[k, c], recv_sem=p_recv.at[slot, c],
            device_id=(g, target, t), device_id_type=pl.DeviceIdType.MESH,
        )

    def relay(k, c):
        @pl.when(outer == 0)
        def _():
            arrived(part_recv.at[k, chunk(c)], p_recv.at[k, c])
            part_send[k, chunk(c), :] = (part[k, chunk(c), :] + part_recv[k, chunk(c), :].astype(f32)).astype(bf16)
            send_part(k, c).start()

    stage = [(spread, 0), (pass_on, 1), (contract, 2)]
    for step in range(nb + 2):
        for run, lag in stage:
            at = step - lag
            if 0 <= at < nb:
                run(order[at])

    for k in (3, 2):
        for c in range(CHUNKS):
            relay(k, c)

    values = column(0, 1)
    for c in range(CHUNKS):
        total = part[0, chunk(c), :]
        for slot in (0, 1):
            arrived(part_recv.at[slot, chunk(c)], p_recv.at[slot, c])
            total = total + part_recv[slot, chunk(c), :].astype(f32)
        gate, up = total[:, :ff], total[:, ff:]
        scale = values[c * piece:(c + 1) * piece]
        hid[b, chunk(c), :] = (gate / (1.0 + jnp.exp(-gate)) * up * scale).astype(bf16)
        for k in (2, 1):
            mine = hid.at[b, chunk(c)]
            remote(mine, mine, h_send.at[k, c], h_recv.at[k, c], blk(k), t)

    def forward(c):
        theirs = hid.at[blk(2), chunk(c)]
        arrived(theirs, h_recv.at[2, c])
        remote(theirs, theirs, h_send.at[3, c], h_recv.at[3, c], blk(1), t)

    def expand(k):
        source = blk(k)
        if k == 0:
            local[2].wait()
        elif k != 2:
            for c in range(CHUNKS):
                arrived(hid.at[source, chunk(c)], h_recv.at[k, c])
        if k == 1:
            for c in range(CHUNKS):
                forward(c)
        routes = column(k, 0)
        h = hid[source].astype(f32)
        routed = jnp.concatenate(
            [jnp.where(routes == e, h, 0.0).astype(bf16) for e in range(experts)], axis=1
        )
        ys[k] = jnp.dot(routed, wd[...].reshape(experts * ff, width), preferred_element_type=f32)
        for j in reversed(range(half)):
            remote(
                ys.at[k, rows_of(tk(pair, 2 * j))], ycore.at[k, j],
                yc_send_sem.at[k, j], yc_recv_sem.at[k, j], b, pair,
            )

    def rows_of(index):
        return pl.ds(pl.multiple_of(index * rows, SUBLANES), rows)

    def exchange(k):
        for j in range(1, half):
            arrived(ycore.at[k, j], yc_recv_sem.at[k, j])
            total = ys[k, rows_of(tk(t, 2 * j)), :] + ycore[k, j]
            yx_send[k, j] = total.astype(bf16)
            remote(
                yx_send.at[k, j], yx_recv.at[k, j],
                yx_send_sem.at[k, j], yx_recv_sem.at[k, j], b, tk(t, 2 * j),
            )

    def finish(k):
        arrived(ycore.at[k, 0], yc_recv_sem.at[k, 0])
        total = ys[k, rows_of(t), :] + ycore[k, 0]
        for j in range(1, half):
            arrived(yx_recv.at[k, j], yx_recv_sem.at[k, j])
            total = total + yx_recv[k, j].astype(f32)
        if k:
            fin_send[k] = total.astype(bf16)
            remote(fin_send.at[k], out_ref.at[:, cols(b)], o_send.at[k], o_recv.at[k], blk(k), t)
        else:
            out_ref[:, cols(b)] = total.astype(bf16)

    stage = [(expand, 0), (exchange, 1), (finish, 2)]
    for step in range(nb + 2):
        for run, lag in stage:
            at = step - lag
            if 0 <= at < nb:
                run(order[at])

    for k in others:
        arrived(out_ref.at[:, cols(blk(k))], o_recv.at[k])
    for copy in sends:
        copy.wait_send()
    for k in others:
        for c in range(CHUNKS):
            send_part(k, c).wait_send()


def stationary_body(nb, nt, tokens, expert_ids, gate_values, w_gate, w_up, w_down):
    rows, features = tokens.shape
    experts, width, ff = w_gate.shape
    f32, bf16 = jnp.float32, jnp.bfloat16
    block, half = nt * rows, nt // 2
    dma = pltpu.SemaphoreType.DMA
    vmem = pl.BlockSpec(memory_space=pltpu.VMEM)
    anywhere = pl.BlockSpec(memory_space=pl.ANY)
    return pl.pallas_call(
        functools.partial(kernel, nb, nt),
        out_shape=jax.ShapeDtypeStruct((rows, features), bf16),
        in_specs=[anywhere, vmem, vmem, anywhere, anywhere, anywhere],
        out_specs=vmem,
        scratch_shapes=[
            pltpu.VMEM((rows, features), bf16),
            pltpu.VMEM((nb, nt, SUBLANES, LANES), f32),
            pltpu.VMEM(w_gate.shape, bf16),
            pltpu.VMEM(w_up.shape, bf16),
            pltpu.VMEM(w_down.shape, bf16),
            pltpu.VMEM((nb, nt, rows, width), bf16),
            pltpu.VMEM((nb, block, 2 * ff), f32),
            pltpu.VMEM((nb, block, 2 * ff), bf16),
            pltpu.VMEM((nb, block, 2 * ff), bf16),
            pltpu.VMEM((nb, block, ff), bf16),
            pltpu.VMEM((nb, block, width), f32),
            pltpu.VMEM((nb, half, rows, width), f32),
            pltpu.VMEM((nb, half, rows, width), bf16),
            pltpu.VMEM((nb, half, rows, width), bf16),
            pltpu.VMEM((nb, rows, width), bf16),
            dma((5,)),
            dma((nb,)), dma((nb,)),
            dma((nb, half)), dma((nb, half)),
            dma((nb,)), dma((nb,)),
            dma((nb, half)), dma((nb, half)),
            dma((nb, nt)), dma((nb, nt)),
            dma((nb, CHUNKS)), dma((nb, CHUNKS)),
            dma((nb, CHUNKS)), dma((nb, CHUNKS)),
            dma((nb, half)), dma((nb, half)),
            dma((nb, half)), dma((nb, half)),
            dma((nb,)), dma((nb,)),
        ],
        compiler_params=pltpu.CompilerParams(collective_id=0, has_side_effects=True),
    )(tokens, expert_ids.reshape(1, rows), gate_values.reshape(1, rows), w_gate, w_up, w_down)


def solution(mesh):
    nb, nt = mesh.shape["blk"], mesh.shape["tok"]

    def body(tokens, expert_ids, gate_values, w_gate, w_up, w_down):
        rows = tokens.shape[0]
        width, ff = w_gate.shape[1], w_gate.shape[2]
        fits = width % LANES == 0 and ff % LANES == 0 and rows % 16 == 0 and rows <= LANES
        if fits and nt % 2 == 0 and nb == 4 and nt * rows % (16 * CHUNKS) == 0:
            return stationary_body(nb, nt, tokens, expert_ids, gate_values, w_gate, w_up, w_down)
        return gathered_body(tokens, expert_ids, gate_values, w_gate, w_up, w_down)

    return jax.shard_map(
        body,
        mesh=mesh,
        in_specs=(
            P(("groups", "blk", "tok"), None),
            P(("groups", "blk", "tok"), None),
            P(("groups", "blk", "tok"), None),
            P(None, "blk", "tok"),
            P(None, "blk", "tok"),
            P(None, "tok", "blk"),
        ),
        out_specs=P(("groups", "blk", "tok"), None),
        check_vma=False,
    )
```

```python
import functools

import jax
import jax.numpy as jnp
from jax import lax
from jax.experimental import pallas as pl
from jax.experimental.pallas import tpu as pltpu
from jax.sharding import PartitionSpec as P

LANES = 128
SUBLANES = 8
CHUNKS = 1
WAVES = 2


def gathered_body(tokens, expert_ids, gate_values, w_gate, w_up, w_down):
    group_rows = lax.all_gather(tokens, "tok", axis=0, tiled=True)
    group_routes = lax.all_gather(expert_ids, "tok", axis=0, tiled=True)[:, 0]
    experts = w_gate.shape[0]
    count_rows = group_rows.shape[0]
    capacity = 3 * count_rows // 4
    expert_range = jnp.arange(experts, dtype=jnp.int32)
    onehot = (group_routes[:, None] == expert_range[None, :]).astype(jnp.int32)
    slot_rank = jnp.sum((jnp.cumsum(onehot, axis=0) - onehot) * onehot, axis=1)
    expert_match = group_routes[None, None, :] == expert_range[:, None, None]
    slot_match = slot_rank[None, None, :] == jnp.arange(capacity, dtype=jnp.int32)[None, :, None]
    dispatch = (expert_match & slot_match).astype(jnp.bfloat16)
    slots = jnp.einsum(
        "esg,gd->esd", dispatch, group_rows, preferred_element_type=jnp.float32
    ).astype(jnp.bfloat16)

    def add_part(weights):
        return jnp.einsum("esd,edf->esf", slots, weights, preferred_element_type=jnp.float32)

    gate_sum = add_part(lax.all_gather(w_gate, "blk", axis=1, tiled=True))
    up_sum = add_part(lax.all_gather(w_up, "blk", axis=1, tiled=True))
    hidden = (jax.nn.silu(gate_sum) * up_sum).astype(jnp.bfloat16)
    slot_out = jnp.einsum(
        "esf,efd->esd",
        hidden,
        lax.all_gather(w_down, "blk", axis=2, tiled=True),
        preferred_element_type=jnp.float32,
    )
    flat_rows = slot_out.reshape(experts * capacity, slot_out.shape[2])
    position = group_routes * capacity + slot_rank
    partial_value = jnp.take(flat_rows, position, axis=0)
    summed = lax.psum_scatter(partial_value, "tok", scatter_dimension=0, tiled=True)
    return (gate_values * summed).astype(jnp.bfloat16)


def kernel(
    nb, nt, tok_hbm, ids_ref, values_ref, wg_hbm, wu_hbm, wd_hbm, out_ref,
    tok, meta, wg, wu, wd, xs, part, part_send, part_recv, hid, ys, ycore, yx_send, yx_recv, fin_send,
    local_sem, z_send, z_recv, x_send, x_recv, c_send, c_recv, f_send, f_recv, m_send, m_recv,
    p_send, p_recv, h_send, h_recv, yc_send_sem, yc_recv_sem, yx_send_sem, yx_recv_sem, o_send, o_recv,
):
    g, b, t = lax.axis_index("groups"), lax.axis_index("blk"), lax.axis_index("tok")
    all_rows, width = tok.shape[0], xs.shape[4]
    rows = all_rows // WAVES
    experts, ff = wg.shape[0], wg.shape[2]
    half = nt // 2
    f32, bf16 = jnp.float32, jnp.bfloat16
    pair = t + 1 - 2 * lax.rem(t, 2)

    outer = lax.rem((b + 1) // 2 + 1, 2)
    piece = nt * rows // CHUNKS

    def blk(k):
        low, high = lax.rem(b, 2), b // 2
        low = 1 - low if k % 2 else low
        high = 1 - high if k // 2 else high
        return 2 * high + low

    def chunk(c):
        return pl.ds(c * piece, piece)

    def tk(base, j):
        return lax.rem(base + j + nt, nt)

    def cols(block):
        return pl.ds(pl.multiple_of(block * width, LANES), width)

    def remote(src, dst, send, recv, to_b, to_t):
        copy = pltpu.make_async_remote_copy(
            src_ref=src, dst_ref=dst, send_sem=send, recv_sem=recv,
            device_id=(g, to_b, to_t), device_id_type=pl.DeviceIdType.MESH,
        )
        copy.start()
        sends.append(copy)

    def arrived(dst, recv):
        pltpu.make_async_copy(dst, dst, recv).wait()

    sends = []
    own = [
        pltpu.make_async_copy(tok_hbm.at[pl.ds(w * rows, rows), cols(b)], xs.at[w, b, t], local_sem.at[5 + w])
        for w in range(WAVES)
    ]
    local = [
        pltpu.make_async_copy(tok_hbm, tok, local_sem.at[0]),
        None,
        pltpu.make_async_copy(wd_hbm, wd, local_sem.at[2]),
        pltpu.make_async_copy(wg_hbm, wg, local_sem.at[3]),
        pltpu.make_async_copy(wu_hbm, wu, local_sem.at[4]),
    ]
    for copy in own + local:
        if copy is not None:
            copy.start()

    meta[b, t] = jnp.zeros((SUBLANES, LANES), f32)
    meta[b, t, 0:1, :all_rows] = ids_ref[...].astype(f32)
    meta[b, t, 1:2, :all_rows] = values_ref[...]

    barrier = pltpu.get_barrier_semaphore()
    for k in range(nb):
        for j in range(nt):
            if k or j:
                pl.semaphore_signal(
                    barrier, inc=1, device_id=(g, blk(k), tk(t, j)),
                    device_id_type=pl.DeviceIdType.MESH,
                )
    pl.semaphore_wait(barrier, nb * nt - 1)

    order = list(range(nb))
    others = order[1:]

    local[0].wait()
    for k in others:
        remote(tok.at[pl.ds(0, rows), cols(blk(k))], xs.at[0, b, t], z_send.at[0, k], z_recv.at[0, k], blk(k), t)
    for k in order:
        for j in range(nt):
            if k or j:
                remote(meta.at[b, t], meta.at[b, t], m_send.at[k, j], m_recv.at[k, j], blk(k), tk(t, j))
    for w in range(1, WAVES):
        for k in others:
            remote(
                tok.at[pl.ds(w * rows, rows), cols(blk(k))], xs.at[w, b, t],
                z_send.at[w, k], z_recv.at[w, k], blk(k), t,
            )
    for copy in own:
        copy.wait()

    def spread(w, k):
        source = blk(k)
        if k:
            arrived(xs.at[w, source, t], z_recv.at[w, k])
        mine = xs.at[w, source, t]
        for j in range(1, half):
            remote(mine, mine, x_send.at[w, k, j], x_recv.at[w, k, j], b, tk(t, 2 * j))
        remote(mine, mine, c_send.at[w, k], c_recv.at[w, k], b, pair)

    def pass_on(w, k):
        source = blk(k)
        for j in range(1, half):
            theirs = xs.at[w, source, tk(t, -2 * j)]
            arrived(theirs, x_recv.at[w, k, j])
            remote(theirs, theirs, f_send.at[w, k, j], f_recv.at[w, k, j], b, pair)

    def column(w, k, row):
        flat = meta[blk(k)].reshape(nt * SUBLANES, LANES)
        turned = jnp.transpose(flat)
        return jnp.concatenate(
            [turned[w * rows:(w + 1) * rows, SUBLANES * i + row:SUBLANES * i + row + 1] for i in range(nt)], axis=0
        )

    def contract(w, k):
        source = blk(k)
        arrived(xs.at[w, source, pair], c_recv.at[w, k])
        for j in range(1, half):
            arrived(xs.at[w, source, tk(pair, -2 * j)], f_recv.at[w, k, j])
        for j in range(nt):
            if w == 0 and (k or j):
                arrived(meta.at[source, tk(t, -j)], m_recv.at[k, j])
        if k == 0 and w == 0:
            local[3].wait()
            local[4].wait()
        routes = column(w, k, 0)
        x = xs[w, source].reshape(nt * rows, width)
        for at, weights in ((0, wg), (ff, wu)):
            total = None
            for e in range(experts):
                value = jnp.dot(x, weights[e], preferred_element_type=f32)
                total = value if e == 0 else jnp.where(routes == e, value, total)
            part[w, k, :, at:at + ff] = total
        if k == 1:
            part_send[w, k] = part[w, k].astype(bf16)
            for c in range(CHUNKS):
                send_part(w, k, c).start()
        elif k:
            @pl.when(outer == 1)
            def _():
                part_send[w, k] = part[w, k].astype(bf16)
                for c in range(CHUNKS):
                    send_part(w, k, c).start()

    def send_part(w, k, c):
        slot = 0 if k == 1 else outer * (5 - k) + 1 - outer
        target = blk(1) if k == 1 else outer * blk(1) + (1 - outer) * blk(k)
        return pltpu.make_async_remote_copy(
            src_ref=part_send.at[w, k, chunk(c)], dst_ref=part_recv.at[w, slot, chunk(c)],
            send_sem=p_send.at[w, k, c], recv_sem=p_recv.at[w, slot, c],
            device_id=(g, target, t), device_id_type=pl.DeviceIdType.MESH,
        )

    def relay(w, k, c):
        @pl.when(outer == 0)
        def _():
            arrived(part_recv.at[w, k, chunk(c)], p_recv.at[w, k, c])
            part_send[w, k, chunk(c), :] = (part[w, k, chunk(c), :] + part_recv[w, k, chunk(c), :].astype(f32)).astype(bf16)
            send_part(w, k, c).start()

    def activate(w):
        values = column(w, 0, 1)
        for c in range(CHUNKS):
            total = part[w, 0, chunk(c), :]
            for slot in (0, 1):
                arrived(part_recv.at[w, slot, chunk(c)], p_recv.at[w, slot, c])
                total = total + part_recv[w, slot, chunk(c), :].astype(f32)
            gate, up = total[:, :ff], total[:, ff:]
            scale = values[c * piece:(c + 1) * piece]
            hid[w, b, chunk(c), :] = (gate / (1.0 + jnp.exp(-gate)) * up * scale).astype(bf16)
            for k in (2, 1):
                mine = hid.at[w, b, chunk(c)]
                remote(mine, mine, h_send.at[w, k, c], h_recv.at[w, k, c], blk(k), t)

    def forward(w, c):
        theirs = hid.at[w, blk(2), chunk(c)]
        arrived(theirs, h_recv.at[w, 2, c])
        remote(theirs, theirs, h_send.at[w, 3, c], h_recv.at[w, 3, c], blk(1), t)

    def expand(w, k):
        source = blk(k)
        if k == 0 and w == 0:
            local[2].wait()
        if k % 2:
            for c in range(CHUNKS):
                arrived(hid.at[w, source, chunk(c)], h_recv.at[w, k, c])
        if k == 1:
            for c in range(CHUNKS):
                forward(w, c)
        routes = column(w, k, 0)
        h = hid[w, source].astype(f32)
        routed = jnp.concatenate(
            [jnp.where(routes == e, h, 0.0).astype(bf16) for e in range(experts)], axis=1
        )
        ys[w, k] = jnp.dot(routed, wd[...].reshape(experts * ff, width), preferred_element_type=f32)
        for j in reversed(range(half)):
            remote(
                ys.at[w, k, rows_of(tk(pair, 2 * j))], ycore.at[w, k, j],
                yc_send_sem.at[w, k, j], yc_recv_sem.at[w, k, j], b, pair,
            )

    def rows_of(index):
        return pl.ds(pl.multiple_of(index * rows, SUBLANES), rows)

    def exchange(w, k):
        for j in range(1, half):
            arrived(ycore.at[w, k, j], yc_recv_sem.at[w, k, j])
            total = ys[w, k, rows_of(tk(t, 2 * j)), :] + ycore[w, k, j]
            yx_send[w, k, j] = total.astype(bf16)
            remote(
                yx_send.at[w, k, j], yx_recv.at[w, k, j],
                yx_send_sem.at[w, k, j], yx_recv_sem.at[w, k, j], b, tk(t, 2 * j),
            )

    def finish(w, k):
        arrived(ycore.at[w, k, 0], yc_recv_sem.at[w, k, 0])
        total = ys[w, k, rows_of(t), :] + ycore[w, k, 0]
        for j in range(1, half):
            arrived(yx_recv.at[w, k, j], yx_recv_sem.at[w, k, j])
            total = total + yx_recv[w, k, j].astype(f32)
        if k:
            fin_send[w, k] = total.astype(bf16)
            remote(fin_send.at[w, k], out_ref.at[pl.ds(w * rows, rows), cols(b)], o_send.at[w, k], o_recv.at[w, k], blk(k), t)
        else:
            out_ref[pl.ds(w * rows, rows), cols(b)] = total.astype(bf16)


    def pipeline(w, stage, fill=()):
        fill = list(fill)
        for step in range(nb + 2):
            for run, lag in stage:
                if 0 <= step - lag < nb:
                    run(w, order[step - lag])
            if fill and step >= 2:
                fill.pop(0)()
        for rest in fill:
            rest()

    def relay_block(w, k):
        for c in range(CHUNKS):
            relay(w, k, c)

    inward = [(spread, 0), (pass_on, 1), (contract, 2)]
    outward = [(expand, 0), (exchange, 1), (finish, 2)]
    for w in range(WAVES):
        fill = []
        if w:
            fill = [functools.partial(relay_block, w - 1, k) for k in (3, 2)]
            fill += [functools.partial(activate, w - 1)]
        pipeline(w, inward, fill)
    for k in (3, 2):
        relay_block(WAVES - 1, k)
    for w in range(WAVES):
        pipeline(w, outward, [functools.partial(activate, WAVES - 1)] if w == 0 else ())

    for w in range(WAVES):
        for k in others:
            arrived(out_ref.at[pl.ds(w * rows, rows), cols(blk(k))], o_recv.at[w, k])
    for copy in sends:
        copy.wait_send()
    for w in range(WAVES):
        for k in others:
            for c in range(CHUNKS):
                send_part(w, k, c).wait_send()


def stationary_body(nb, nt, tokens, expert_ids, gate_values, w_gate, w_up, w_down):
    rows, features = tokens.shape
    experts, width, ff = w_gate.shape
    f32, bf16 = jnp.float32, jnp.bfloat16
    wave_rows = rows // WAVES
    block, half = nt * wave_rows, nt // 2
    dma = pltpu.SemaphoreType.DMA
    vmem = pl.BlockSpec(memory_space=pltpu.VMEM)
    anywhere = pl.BlockSpec(memory_space=pl.ANY)
    return pl.pallas_call(
        functools.partial(kernel, nb, nt),
        out_shape=jax.ShapeDtypeStruct((rows, features), bf16),
        in_specs=[anywhere, vmem, vmem, anywhere, anywhere, anywhere],
        out_specs=vmem,
        scratch_shapes=[
            pltpu.VMEM((rows, features), bf16),
            pltpu.VMEM((nb, nt, SUBLANES, LANES), f32),
            pltpu.VMEM(w_gate.shape, bf16),
            pltpu.VMEM(w_up.shape, bf16),
            pltpu.VMEM(w_down.shape, bf16),
            pltpu.VMEM((WAVES, nb, nt, wave_rows, width), bf16),
            pltpu.VMEM((WAVES, nb, block, 2 * ff), f32),
            pltpu.VMEM((WAVES, nb, block, 2 * ff), bf16),
            pltpu.VMEM((WAVES, nb, block, 2 * ff), bf16),
            pltpu.VMEM((WAVES, nb, block, ff), bf16),
            pltpu.VMEM((WAVES, nb, block, width), f32),
            pltpu.VMEM((WAVES, nb, half, wave_rows, width), f32),
            pltpu.VMEM((WAVES, nb, half, wave_rows, width), bf16),
            pltpu.VMEM((WAVES, nb, half, wave_rows, width), bf16),
            pltpu.VMEM((WAVES, nb, wave_rows, width), bf16),
            dma((5 + WAVES,)),
            dma((WAVES, nb,)), dma((WAVES, nb,)),
            dma((WAVES, nb, half)), dma((WAVES, nb, half)),
            dma((WAVES, nb,)), dma((WAVES, nb,)),
            dma((WAVES, nb, half)), dma((WAVES, nb, half)),
            dma((nb, nt)), dma((nb, nt)),
            dma((WAVES, nb, CHUNKS)), dma((WAVES, nb, CHUNKS)),
            dma((WAVES, nb, CHUNKS)), dma((WAVES, nb, CHUNKS)),
            dma((WAVES, nb, half)), dma((WAVES, nb, half)),
            dma((WAVES, nb, half)), dma((WAVES, nb, half)),
            dma((WAVES, nb,)), dma((WAVES, nb,)),
        ],
        compiler_params=pltpu.CompilerParams(collective_id=0, has_side_effects=True),
    )(tokens, expert_ids.reshape(1, rows), gate_values.reshape(1, rows), w_gate, w_up, w_down)


def solution(mesh):
    nb, nt = mesh.shape["blk"], mesh.shape["tok"]

    def body(tokens, expert_ids, gate_values, w_gate, w_up, w_down):
        rows = tokens.shape[0]
        width, ff = w_gate.shape[1], w_gate.shape[2]
        fits = width % LANES == 0 and ff % LANES == 0 and rows % (16 * WAVES) == 0 and rows <= LANES
        if fits and nt % 2 == 0 and nb == 4 and nt * rows % (16 * CHUNKS * WAVES) == 0:
            return stationary_body(nb, nt, tokens, expert_ids, gate_values, w_gate, w_up, w_down)
        return gathered_body(tokens, expert_ids, gate_values, w_gate, w_up, w_down)

    return jax.shard_map(
        body,
        mesh=mesh,
        in_specs=(
            P(("groups", "blk", "tok"), None),
            P(("groups", "blk", "tok"), None),
            P(("groups", "blk", "tok"), None),
            P(None, "blk", "tok"),
            P(None, "blk", "tok"),
            P(None, "tok", "blk"),
        ),
        out_specs=P(("groups", "blk", "tok"), None),
        check_vma=False,
    )
```

```python
import functools

import jax
import jax.numpy as jnp
from jax import lax
from jax.experimental import pallas as pl
from jax.experimental.pallas import tpu as pltpu
from jax.sharding import PartitionSpec as P

LANES = 128
SUBLANES = 8
CHUNKS = 1
WAVES = 4


def gathered_body(tokens, expert_ids, gate_values, w_gate, w_up, w_down):
    group_rows = lax.all_gather(tokens, "tok", axis=0, tiled=True)
    group_routes = lax.all_gather(expert_ids, "tok", axis=0, tiled=True)[:, 0]
    experts = w_gate.shape[0]
    count_rows = group_rows.shape[0]
    capacity = 3 * count_rows // 4
    expert_range = jnp.arange(experts, dtype=jnp.int32)
    onehot = (group_routes[:, None] == expert_range[None, :]).astype(jnp.int32)
    slot_rank = jnp.sum((jnp.cumsum(onehot, axis=0) - onehot) * onehot, axis=1)
    expert_match = group_routes[None, None, :] == expert_range[:, None, None]
    slot_match = slot_rank[None, None, :] == jnp.arange(capacity, dtype=jnp.int32)[None, :, None]
    dispatch = (expert_match & slot_match).astype(jnp.bfloat16)
    slots = jnp.einsum(
        "esg,gd->esd", dispatch, group_rows, preferred_element_type=jnp.float32
    ).astype(jnp.bfloat16)

    def add_part(weights):
        return jnp.einsum("esd,edf->esf", slots, weights, preferred_element_type=jnp.float32)

    gate_sum = add_part(lax.all_gather(w_gate, "blk", axis=1, tiled=True))
    up_sum = add_part(lax.all_gather(w_up, "blk", axis=1, tiled=True))
    hidden = (jax.nn.silu(gate_sum) * up_sum).astype(jnp.bfloat16)
    slot_out = jnp.einsum(
        "esf,efd->esd",
        hidden,
        lax.all_gather(w_down, "blk", axis=2, tiled=True),
        preferred_element_type=jnp.float32,
    )
    flat_rows = slot_out.reshape(experts * capacity, slot_out.shape[2])
    position = group_routes * capacity + slot_rank
    partial_value = jnp.take(flat_rows, position, axis=0)
    summed = lax.psum_scatter(partial_value, "tok", scatter_dimension=0, tiled=True)
    return (gate_values * summed).astype(jnp.bfloat16)


def kernel(
    nb, nt, tok_hbm, ids_ref, values_ref, wg_hbm, wu_hbm, wd_hbm, out_ref,
    tok, meta, wg, wu, wd, xs, part, part_send, part_recv, hid, ys, ycore, yx_send, yx_recv, fin_send,
    local_sem, z_send, z_recv, x_send, x_recv, c_send, c_recv, f_send, f_recv, m_send, m_recv,
    p_send, p_recv, h_send, h_recv, yc_send_sem, yc_recv_sem, yx_send_sem, yx_recv_sem, o_send, o_recv,
):
    g, b, t = lax.axis_index("groups"), lax.axis_index("blk"), lax.axis_index("tok")
    all_rows, width = tok.shape[0], xs.shape[4]
    rows = all_rows // WAVES
    experts, ff = wg.shape[0], wg.shape[2]
    half = nt // 2
    f32, bf16 = jnp.float32, jnp.bfloat16
    pair = t + 1 - 2 * lax.rem(t, 2)

    outer = lax.rem((b + 1) // 2 + 1, 2)
    piece = nt * rows // CHUNKS

    def blk(k):
        low, high = lax.rem(b, 2), b // 2
        low = 1 - low if k % 2 else low
        high = 1 - high if k // 2 else high
        return 2 * high + low

    def chunk(c):
        return pl.ds(c * piece, piece)

    def tk(base, j):
        return lax.rem(base + j + nt, nt)

    def cols(block):
        return pl.ds(pl.multiple_of(block * width, LANES), width)

    def remote(src, dst, send, recv, to_b, to_t):
        copy = pltpu.make_async_remote_copy(
            src_ref=src, dst_ref=dst, send_sem=send, recv_sem=recv,
            device_id=(g, to_b, to_t), device_id_type=pl.DeviceIdType.MESH,
        )
        copy.start()
        sends.append(copy)

    def arrived(dst, recv):
        pltpu.make_async_copy(dst, dst, recv).wait()

    sends = []
    own = [
        pltpu.make_async_copy(tok_hbm.at[pl.ds(w * rows, rows), cols(b)], xs.at[w, b, t], local_sem.at[5 + w])
        for w in range(WAVES)
    ]
    local = [
        pltpu.make_async_copy(tok_hbm, tok, local_sem.at[0]),
        None,
        pltpu.make_async_copy(wd_hbm, wd, local_sem.at[2]),
        pltpu.make_async_copy(wg_hbm, wg, local_sem.at[3]),
        pltpu.make_async_copy(wu_hbm, wu, local_sem.at[4]),
    ]
    for copy in own + local:
        if copy is not None:
            copy.start()

    meta[b, t] = jnp.zeros((SUBLANES, LANES), f32)
    meta[b, t, 0:1, :all_rows] = ids_ref[...].astype(f32)
    meta[b, t, 1:2, :all_rows] = values_ref[...]

    barrier = pltpu.get_barrier_semaphore()
    for k in range(nb):
        for j in range(nt):
            if k or j:
                pl.semaphore_signal(
                    barrier, inc=1, device_id=(g, blk(k), tk(t, j)),
                    device_id_type=pl.DeviceIdType.MESH,
                )
    pl.semaphore_wait(barrier, nb * nt - 1)

    order = list(range(nb))
    others = order[1:]

    local[0].wait()
    for k in others:
        remote(tok.at[pl.ds(0, rows), cols(blk(k))], xs.at[0, b, t], z_send.at[0, k], z_recv.at[0, k], blk(k), t)
    for k in order:
        for j in range(nt):
            if k or j:
                remote(meta.at[b, t], meta.at[b, t], m_send.at[k, j], m_recv.at[k, j], blk(k), tk(t, j))
    for w in range(1, WAVES):
        for k in others:
            remote(
                tok.at[pl.ds(w * rows, rows), cols(blk(k))], xs.at[w, b, t],
                z_send.at[w, k], z_recv.at[w, k], blk(k), t,
            )
    for copy in own:
        copy.wait()

    def spread(w, k):
        source = blk(k)
        if k:
            arrived(xs.at[w, source, t], z_recv.at[w, k])
        mine = xs.at[w, source, t]
        for j in range(1, half):
            remote(mine, mine, x_send.at[w, k, j], x_recv.at[w, k, j], b, tk(t, 2 * j))
        remote(mine, mine, c_send.at[w, k], c_recv.at[w, k], b, pair)

    def pass_on(w, k):
        source = blk(k)
        for j in range(1, half):
            theirs = xs.at[w, source, tk(t, -2 * j)]
            arrived(theirs, x_recv.at[w, k, j])
            remote(theirs, theirs, f_send.at[w, k, j], f_recv.at[w, k, j], b, pair)

    def column(w, k, row):
        flat = meta[blk(k)].reshape(nt * SUBLANES, LANES)
        turned = jnp.transpose(flat)
        return jnp.concatenate(
            [turned[w * rows:(w + 1) * rows, SUBLANES * i + row:SUBLANES * i + row + 1] for i in range(nt)], axis=0
        )

    def contract(w, k):
        source = blk(k)
        arrived(xs.at[w, source, pair], c_recv.at[w, k])
        for j in range(1, half):
            arrived(xs.at[w, source, tk(pair, -2 * j)], f_recv.at[w, k, j])
        for j in range(nt):
            if w == 0 and (k or j):
                arrived(meta.at[source, tk(t, -j)], m_recv.at[k, j])
        if k == 0 and w == 0:
            local[3].wait()
            local[4].wait()
        routes = column(w, k, 0)
        x = xs[w, source].reshape(nt * rows, width)
        for at, weights in ((0, wg), (ff, wu)):
            total = None
            for e in range(experts):
                value = jnp.dot(x, weights[e], preferred_element_type=f32)
                total = value if e == 0 else jnp.where(routes == e, value, total)
            part[w, k, :, at:at + ff] = total
        if k == 1:
            part_send[w, k] = part[w, k].astype(bf16)
            for c in range(CHUNKS):
                send_part(w, k, c).start()
        elif k:
            @pl.when(outer == 1)
            def _():
                part_send[w, k] = part[w, k].astype(bf16)
                for c in range(CHUNKS):
                    send_part(w, k, c).start()

    def send_part(w, k, c):
        slot = 0 if k == 1 else outer * (5 - k) + 1 - outer
        target = blk(1) if k == 1 else outer * blk(1) + (1 - outer) * blk(k)
        return pltpu.make_async_remote_copy(
            src_ref=part_send.at[w, k, chunk(c)], dst_ref=part_recv.at[w, slot, chunk(c)],
            send_sem=p_send.at[w, k, c], recv_sem=p_recv.at[w, slot, c],
            device_id=(g, target, t), device_id_type=pl.DeviceIdType.MESH,
        )

    def relay(w, k, c):
        @pl.when(outer == 0)
        def _():
            arrived(part_recv.at[w, k, chunk(c)], p_recv.at[w, k, c])
            part_send[w, k, chunk(c), :] = (part[w, k, chunk(c), :] + part_recv[w, k, chunk(c), :].astype(f32)).astype(bf16)
            send_part(w, k, c).start()

    def activate(w):
        values = column(w, 0, 1)
        for c in range(CHUNKS):
            total = part[w, 0, chunk(c), :]
            for slot in (0, 1):
                arrived(part_recv.at[w, slot, chunk(c)], p_recv.at[w, slot, c])
                total = total + part_recv[w, slot, chunk(c), :].astype(f32)
            gate, up = total[:, :ff], total[:, ff:]
            scale = values[c * piece:(c + 1) * piece]
            hid[w, b, chunk(c), :] = (gate / (1.0 + jnp.exp(-gate)) * up * scale).astype(bf16)
            for k in (2, 1):
                mine = hid.at[w, b, chunk(c)]
                remote(mine, mine, h_send.at[w, k, c], h_recv.at[w, k, c], blk(k), t)

    def forward(w, c):
        theirs = hid.at[w, blk(2), chunk(c)]
        arrived(theirs, h_recv.at[w, 2, c])
        remote(theirs, theirs, h_send.at[w, 3, c], h_recv.at[w, 3, c], blk(1), t)

    def expand(w, k):
        source = blk(k)
        if k == 0 and w == 0:
            local[2].wait()
        if k % 2:
            for c in range(CHUNKS):
                arrived(hid.at[w, source, chunk(c)], h_recv.at[w, k, c])
        if k == 1:
            for c in range(CHUNKS):
                forward(w, c)
        routes = column(w, k, 0)
        h = hid[w, source].astype(f32)
        routed = jnp.concatenate(
            [jnp.where(routes == e, h, 0.0).astype(bf16) for e in range(experts)], axis=1
        )
        ys[w, k] = jnp.dot(routed, wd[...].reshape(experts * ff, width), preferred_element_type=f32)
        for j in reversed(range(half)):
            remote(
                ys.at[w, k, rows_of(tk(pair, 2 * j))], ycore.at[w, k, j],
                yc_send_sem.at[w, k, j], yc_recv_sem.at[w, k, j], b, pair,
            )

    def rows_of(index):
        return pl.ds(pl.multiple_of(index * rows, SUBLANES), rows)

    def exchange(w, k):
        for j in range(1, half):
            arrived(ycore.at[w, k, j], yc_recv_sem.at[w, k, j])
            total = ys[w, k, rows_of(tk(t, 2 * j)), :] + ycore[w, k, j]
            yx_send[w, k, j] = total.astype(bf16)
            remote(
                yx_send.at[w, k, j], yx_recv.at[w, k, j],
                yx_send_sem.at[w, k, j], yx_recv_sem.at[w, k, j], b, tk(t, 2 * j),
            )

    def finish(w, k):
        arrived(ycore.at[w, k, 0], yc_recv_sem.at[w, k, 0])
        total = ys[w, k, rows_of(t), :] + ycore[w, k, 0]
        for j in range(1, half):
            arrived(yx_recv.at[w, k, j], yx_recv_sem.at[w, k, j])
            total = total + yx_recv[w, k, j].astype(f32)
        if k:
            fin_send[w, k] = total.astype(bf16)
            remote(fin_send.at[w, k], out_ref.at[pl.ds(w * rows, rows), cols(b)], o_send.at[w, k], o_recv.at[w, k], blk(k), t)
        else:
            out_ref[pl.ds(w * rows, rows), cols(b)] = total.astype(bf16)


    def pipeline(w, stage, fill=()):
        fill = list(fill)
        for step in range(nb + 2):
            for run, lag in stage:
                if 0 <= step - lag < nb:
                    run(w, order[step - lag])
            if fill and step >= 2:
                fill.pop(0)()
        for rest in fill:
            rest()

    def relay_block(w, k):
        for c in range(CHUNKS):
            relay(w, k, c)

    inward = [(spread, 0), (pass_on, 1), (contract, 2)]
    outward = [(expand, 0), (exchange, 1), (finish, 2)]
    for w in range(WAVES):
        fill = []
        if w:
            fill = [functools.partial(relay_block, w - 1, k) for k in (3, 2)]
            fill += [functools.partial(activate, w - 1)]
        pipeline(w, inward, fill)
    for k in (3, 2):
        relay_block(WAVES - 1, k)
    for w in range(WAVES):
        pipeline(w, outward, [functools.partial(activate, WAVES - 1)] if w == 0 else ())

    for w in range(WAVES):
        for k in others:
            arrived(out_ref.at[pl.ds(w * rows, rows), cols(blk(k))], o_recv.at[w, k])
    for copy in sends:
        copy.wait_send()
    for w in range(WAVES):
        for k in others:
            for c in range(CHUNKS):
                send_part(w, k, c).wait_send()


def stationary_body(nb, nt, tokens, expert_ids, gate_values, w_gate, w_up, w_down):
    rows, features = tokens.shape
    experts, width, ff = w_gate.shape
    f32, bf16 = jnp.float32, jnp.bfloat16
    wave_rows = rows // WAVES
    block, half = nt * wave_rows, nt // 2
    dma = pltpu.SemaphoreType.DMA
    vmem = pl.BlockSpec(memory_space=pltpu.VMEM)
    anywhere = pl.BlockSpec(memory_space=pl.ANY)
    return pl.pallas_call(
        functools.partial(kernel, nb, nt),
        out_shape=jax.ShapeDtypeStruct((rows, features), bf16),
        in_specs=[anywhere, vmem, vmem, anywhere, anywhere, anywhere],
        out_specs=vmem,
        scratch_shapes=[
            pltpu.VMEM((rows, features), bf16),
            pltpu.VMEM((nb, nt, SUBLANES, LANES), f32),
            pltpu.VMEM(w_gate.shape, bf16),
            pltpu.VMEM(w_up.shape, bf16),
            pltpu.VMEM(w_down.shape, bf16),
            pltpu.VMEM((WAVES, nb, nt, wave_rows, width), bf16),
            pltpu.VMEM((WAVES, nb, block, 2 * ff), f32),
            pltpu.VMEM((WAVES, nb, block, 2 * ff), bf16),
            pltpu.VMEM((WAVES, nb, block, 2 * ff), bf16),
            pltpu.VMEM((WAVES, nb, block, ff), bf16),
            pltpu.VMEM((WAVES, nb, block, width), f32),
            pltpu.VMEM((WAVES, nb, half, wave_rows, width), f32),
            pltpu.VMEM((WAVES, nb, half, wave_rows, width), bf16),
            pltpu.VMEM((WAVES, nb, half, wave_rows, width), bf16),
            pltpu.VMEM((WAVES, nb, wave_rows, width), bf16),
            dma((5 + WAVES,)),
            dma((WAVES, nb,)), dma((WAVES, nb,)),
            dma((WAVES, nb, half)), dma((WAVES, nb, half)),
            dma((WAVES, nb,)), dma((WAVES, nb,)),
            dma((WAVES, nb, half)), dma((WAVES, nb, half)),
            dma((nb, nt)), dma((nb, nt)),
            dma((WAVES, nb, CHUNKS)), dma((WAVES, nb, CHUNKS)),
            dma((WAVES, nb, CHUNKS)), dma((WAVES, nb, CHUNKS)),
            dma((WAVES, nb, half)), dma((WAVES, nb, half)),
            dma((WAVES, nb, half)), dma((WAVES, nb, half)),
            dma((WAVES, nb,)), dma((WAVES, nb,)),
        ],
        compiler_params=pltpu.CompilerParams(collective_id=0, has_side_effects=True),
    )(tokens, expert_ids.reshape(1, rows), gate_values.reshape(1, rows), w_gate, w_up, w_down)


def solution(mesh):
    nb, nt = mesh.shape["blk"], mesh.shape["tok"]

    def body(tokens, expert_ids, gate_values, w_gate, w_up, w_down):
        rows = tokens.shape[0]
        width, ff = w_gate.shape[1], w_gate.shape[2]
        fits = width % LANES == 0 and ff % LANES == 0 and rows % (16 * WAVES) == 0 and rows <= LANES
        if fits and nt % 2 == 0 and nb == 4 and nt * rows % (16 * CHUNKS * WAVES) == 0:
            return stationary_body(nb, nt, tokens, expert_ids, gate_values, w_gate, w_up, w_down)
        return gathered_body(tokens, expert_ids, gate_values, w_gate, w_up, w_down)

    return jax.shard_map(
        body,
        mesh=mesh,
        in_specs=(
            P(("groups", "blk", "tok"), None),
            P(("groups", "blk", "tok"), None),
            P(("groups", "blk", "tok"), None),
            P(None, "blk", "tok"),
            P(None, "blk", "tok"),
            P(None, "tok", "blk"),
        ),
        out_specs=P(("groups", "blk", "tok"), None),
        check_vma=False,
    )
```
